32 devices in a mesh: fsdp: 8 (over z, y), tp: 4 (over x, core).
Axes of the slice: x: 2, y: 2, z: 4, core: 2. Of those that a mesh axis runs over, the one named last changes fastest.
Arguments:
- base_o: bfloat16 [2, 8192, 8192], P(None, 'tp', 'fsdp'), may hold values from -0.0625 to 0.0625
- base_down: bfloat16 [2, 28672, 8192], P(None, 'tp', 'fsdp'), may hold values from -0.03125 to 0.03125
- factor_a_o: bfloat16 [2, 64, 4, 2048], P(None, None, None, 'fsdp'), may hold values from -0.0625 to 0.0625
- factor_b_o: bfloat16 [2, 8192, 64], P(None, 'fsdp'), may hold values from -1.1953125 to 1.1953125
- factor_a_down: bfloat16 [2, 64, 4, 7168], P(None, None, None, 'fsdp'), may hold values from -0.03125 to 0.03125
- factor_b_down: bfloat16 [2, 8192, 64], P(None, 'fsdp'), may hold values from -1.1953125 to 1.1953125
- magnitude_o: float32 [2, 8192], P(None, 'fsdp'), may hold values from 30 to 300
- magnitude_down: float32 [2, 8192], P(None, 'fsdp'), may hold values from 30 to 300
Outputs:
- merged_o: bfloat16 [2, 8192, 8192], P(None, 'tp', 'fsdp')
- merged_down: bfloat16 [2, 28672, 8192], P(None, 'tp', 'fsdp')
The draws below stay inside these ranges and needn't reach their ends.
All inputs are finite; a program needn't handle non-finite values.
Results may differ from the reference program's by a relative error of at most 0.001.
Values may be sent and summed in bfloat16 or wider, within the bound.
A program may use at most 192 MiB of HBM per device.

```python
import math
import jax
import jax.numpy as jnp
from jax import lax

D = 8192
FF = 28672
R = 64
LAYERS = 2
N_TP = 4


def level_of(rng, dims, cuts, smallest, top_value):
    def one(dim, shards_of):
        steps = jax.random.uniform(jax.random.fold_in(jax.random.fold_in(rng, 6), dim), (shards_of,), jnp.float32, smallest / len(cuts), top_value / len(cuts))
        return jnp.repeat(jnp.exp(steps), dims[dim] // shards_of).reshape((-1,) + (1,) * (len(dims) - dim - 1))

    level = one(*cuts[0])
    for cut in cuts[1:]:
        level = level * one(*cut)
    return level


def noise(stream_key, extent, width, reach, split=(), dtype=jnp.bfloat16):
    gain = level_of(stream_key, extent, split, -0.22, 0.18) if split else 1.0
    drawn = jax.random.normal(stream_key, extent, jnp.float32) * width * gain
    return jnp.minimum(jnp.maximum(drawn, -reach), reach).astype(dtype)


def setup_inputs(seed: int = 0) -> dict:
    seeds = jax.random.split(jax.random.key(seed), 9)
    return {
        "base_o": noise(seeds[0], (LAYERS, D, D), D ** -0.5, 0.0625, ((1, 4), (2, 8))),
        "base_down": noise(seeds[1], (LAYERS, FF, D), FF ** -0.5, 0.03125, ((1, 4), (2, 8))),
        "factor_a_o": noise(seeds[2], (LAYERS, R, N_TP, D // N_TP), D ** -0.5, 0.0625, ((3, 8),)),
        "factor_b_o": noise(seeds[3], (LAYERS, D, R), 0.2, 1.1953125, ((1, 8),)),
        "factor_a_down": noise(seeds[4], (LAYERS, R, N_TP, FF // N_TP), FF ** -0.5, 0.03125, ((3, 8),)),
        "factor_b_down": noise(seeds[5], (LAYERS, D, R), 0.2, 1.1953125, ((1, 8),)),
        "magnitude_o": jnp.clip(jnp.exp(math.log(300.0) - 2.3025851 * jax.random.uniform(seeds[6], (LAYERS, D), jnp.float32) ** level_of(seeds[6], (LAYERS, D), ((1, 8),), -0.2, 0.2)), 30.0, 300.0),
        "magnitude_down": jnp.clip(jnp.exp(math.log(300.0) - 2.3025851 * jax.random.uniform(seeds[7], (LAYERS, D), jnp.float32) ** level_of(seeds[7], (LAYERS, D), ((1, 8),), -0.2, 0.2)), 30.0, 300.0),
    }


def refresh(base, factor_a, factor_b, magnitude):
    full_a = factor_a.reshape(factor_a.shape[0], factor_a.shape[1], -1)

    def single(items):
        base_layer, a_layer, b_layer, m_layer = items
        delta = jnp.dot(a_layer.T, b_layer.T, preferred_element_type=jnp.float32)
        summed = base_layer.astype(jnp.float32) + 0.25 * delta
        square = lax.optimization_barrier(jnp.sum(summed * summed, axis=0))
        return (m_layer[None, :] * summed * lax.rsqrt(square + 1e-06)[None, :]).astype(jnp.bfloat16)
    return lax.map(single, (base, full_a, factor_b, magnitude))

def reference(base_o, base_down, factor_a_o, factor_b_o, factor_a_down, factor_b_down, magnitude_o, magnitude_down):
    merged_o = refresh(base_o, factor_a_o, factor_b_o, magnitude_o)
    merged_down = refresh(base_down, factor_a_down, factor_b_down, magnitude_down)
    return (merged_o, merged_down)
```

```python
import functools

import jax
import jax.numpy as jnp
from jax import lax
from jax.experimental import pallas as pl
from jax.experimental.pallas import tpu as pltpu
from jax.sharding import PartitionSpec as P

MESH = pl.DeviceIdType.MESH
F32 = jnp.float32
BF16 = jnp.bfloat16


def row_tile(rows, most):
    return max(t for t in range(16, most + 1, 16) if rows % t == 0)


def gather_kernel(
    n,
    n_tp,
    sizes,
    rank,
    base_o,
    base_d,
    a_o,
    a_d,
    b_o,
    b_d,
    mag_o,
    mag_d,
    held_o,
    held_d,
    full_a,
    weights,
    scale,
    block,
    acc,
    sums,
    peers,
    read_sem,
    own_sem,
    send_sem,
    recv_sem,
    sum_send,
    sum_recv,
):
    layers, columns = mag_o.shape
    depth = n // 2
    me, t = lax.axis_index("fsdp"), lax.axis_index("tp")
    z, y = me // 2, me % 2
    other = z * 2 + 1 - y
    has_lo, has_hi = z > 0, z < depth - 1

    def to_fsdp(f):
        return {"fsdp": f}

    barrier = pltpu.get_barrier_semaphore()

    def greet(device):
        pl.semaphore_signal(barrier, inc=1, device_id=device, device_id_type=MESH)

    greet(to_fsdp(other))
    for k in range(1, n_tp):
        greet({"tp": (t + k) % n_tp})
    pl.when(has_lo)(lambda: greet(to_fsdp(me - 2)))
    pl.when(has_hi)(lambda: greet(to_fsdp(me + 2)))

    def slot_of(e, lo, side):
        return (z - e if lo else z + e) * 2 + side

    bases = (base_o, base_d)
    helds = (held_o, held_d)
    starts = (0, sizes[0])

    def read(p, layer, f):
        rows = pl.ds(pl.multiple_of(f * sizes[p], 16), sizes[p])
        return pltpu.make_async_copy(
            bases[p].at[layer, rows], helds[p].at[layer, rows], read_sem.at[p, layer, f]
        )

    def read_slot(f):
        for p in range(2):
            for layer in range(layers):
                read(p, layer, f).start()

    read_slot(me)
    read_slot(other)

    @pl.loop(1, depth)
    def _(d):
        for side in (y, 1 - y):
            pl.when(z - d >= 0)(lambda: read_slot(slot_of(d, True, side)))
            pl.when(z + d < depth)(lambda: read_slot(slot_of(d, False, side)))

    for p, a in enumerate((a_o, a_d)):
        parts = []
        for layer in range(layers):
            rows = a[layer, :, 0, :].astype(F32)
            for u in range(1, n_tp):
                rows = jnp.where(t == u, a[layer, :, u, :].astype(F32), rows)
            parts.append(rows)
        block[pl.ds(starts[p], sizes[p]), :] = jnp.concatenate(parts, axis=0).T.astype(BF16)

    ends = has_lo.astype(jnp.int32) + has_hi.astype(jnp.int32)
    pl.semaphore_wait(barrier, n_tp + ends)

    def send(source, f, way, target):
        return pltpu.make_async_remote_copy(
            src_ref=source,
            dst_ref=full_a.at[f],
            send_sem=send_sem.at[way, f],
            recv_sem=recv_sem.at[f],
            device_id=to_fsdp(target),
            device_id_type=MESH,
        )

    def arrived(f):
        send(full_a.at[f], f, 0, other).wait_recv()

    pl.when(has_lo)(lambda: send(block, me, 1, me - 2).start())
    pl.when(has_hi)(lambda: send(block, me, 2, me + 2).start())
    send(block, me, 0, other).start()
    own = pltpu.make_async_copy(block, full_a.at[me], own_sem)
    own.start()

    for p, b in enumerate((b_o, b_d)):
        for layer in range(layers):
            weights[p, layer] = jnp.zeros((layers * rank, columns), BF16)
            weights[p, layer, pl.ds(layer * rank, rank), :] = (
                b[layer].astype(F32) * 0.25
            ).astype(BF16)
    acc[...] = jnp.zeros_like(acc)
    own.wait()

    wide = 256 if columns % 256 == 0 else columns

    def process(f):
        for p in range(2):
            tile = row_tile(sizes[p], 256)

            @pl.loop(0, layers)
            def _(layer):
                read(p, layer, f).wait()

                @pl.loop(0, sizes[p] // tile)
                def _(i):
                    rows = pl.ds(pl.multiple_of(starts[p] + i * tile, 16), tile)
                    held = pl.ds(pl.multiple_of(f * sizes[p] + i * tile, 16), tile)
                    left = full_a[f, rows, :]
                    for c in range(0, columns, wide):
                        cut = pl.ds(c, wide)
                        total = jnp.dot(
                            left, weights[p, layer, :, cut], preferred_element_type=F32
                        ) + helds[p][layer, held, cut].astype(F32)
                        acc[p, layer, :, cut] += jnp.sum(
                            (total * total).reshape(tile // 8, 8, wide), axis=0
                        )

    def from_other(e):
        def take(f):
            arrived(f)
            process(f)

        pl.when(z - e >= 0)(lambda: take(slot_of(e, True, 1 - y)))
        pl.when((e > 0) & (z + e < depth))(lambda: take(slot_of(e, False, 1 - y)))

    process(me)

    @pl.loop(1, depth)
    def _(d):
        @pl.when(z - d >= 0)
        def _():
            f = slot_of(d, True, y)
            arrived(f)
            pl.when(has_hi)(lambda: send(full_a.at[f], f, 2, me + 2).start())
            send(full_a.at[f], f, 0, other).start()

        @pl.when(z + d < depth)
        def _():
            f = slot_of(d, False, y)
            arrived(f)
            pl.when(has_lo)(lambda: send(full_a.at[f], f, 1, me - 2).start())
            send(full_a.at[f], f, 0, other).start()

        from_other(d - 1)
        pl.when(z - d >= 0)(lambda: process(slot_of(d, True, y)))
        pl.when(z + d < depth)(lambda: process(slot_of(d, False, y)))

    from_other(jnp.int32(depth - 1))

    for p in range(2):
        for layer in range(layers):
            sums[p * layers + layer, :] = jnp.sum(acc[p, layer], axis=0)

    pl.when(has_lo)(lambda: send(block, me, 1, me - 2).wait_send())
    pl.when(has_hi)(lambda: send(block, me, 2, me + 2).wait_send())
    send(block, me, 0, other).wait_send()

    @pl.loop(1, depth)
    def _(d):
        @pl.when(z - d >= 0)
        def _():
            f = slot_of(d, True, y)
            pl.when(has_hi)(lambda: send(full_a.at[f], f, 2, me + 2).wait_send())
            send(full_a.at[f], f, 0, other).wait_send()

        @pl.when(z + d < depth)
        def _():
            f = slot_of(d, False, y)
            pl.when(has_lo)(lambda: send(full_a.at[f], f, 1, me - 2).wait_send())
            send(full_a.at[f], f, 0, other).wait_send()

    def share(k):
        return pltpu.make_async_remote_copy(
            src_ref=sums,
            dst_ref=peers.at[k - 1],
            send_sem=sum_send.at[k - 1],
            recv_sem=sum_recv.at[k - 1],
            device_id={"tp": (t + k) % n_tp},
            device_id_type=MESH,
        )

    for k in range(1, n_tp):
        share(k).start()
    square = sums[...]
    for k in range(1, n_tp):
        share(k).wait()
    for k in range(1, n_tp):
        square = square + peers[k - 1]
    magnitude = jnp.concatenate([mag_o[...], mag_d[...]], axis=0)
    scale[...] = magnitude * lax.rsqrt(square + 1e-06)


def finish_kernel(sizes, held_o, held_d, full_a, weights, scale, out_o, out_d):
    layers, _, columns = held_o.shape
    layer, f = pl.program_id(0), pl.program_id(1)
    wide = 256 if columns % 256 == 0 else columns
    for p, (held, out) in enumerate(((held_o, out_o), (held_d, out_d))):
        size, start = sizes[p], sum(sizes[:p])
        tile = row_tile(size, 256)
        factor = scale[pl.ds(p * layers + layer, 1), :]

        @pl.loop(0, size // tile)
        def _(i):
            rows = pl.ds(pl.multiple_of(start + i * tile, 16), tile)
            inside = pl.ds(pl.multiple_of(f * size + i * tile, 16), tile)
            here = pl.ds(pl.multiple_of(i * tile, 16), tile)
            left = full_a[f, rows, :]
            for c in range(0, columns, wide):
                cut = pl.ds(c, wide)
                total = jnp.dot(
                    left, weights[p, layer, :, cut], preferred_element_type=F32
                ) + held[layer, inside, cut].astype(F32)
                out[0, here, cut] = (total * factor[:, c : c + wide]).astype(BF16)


def solution(mesh):
    n, n_tp = mesh.shape["fsdp"], mesh.shape["tp"]
    in_vmem = pl.BlockSpec(memory_space=pltpu.VMEM)
    anywhere = pl.BlockSpec(memory_space=pl.ANY)

    def local(base_o, base_d, a_o, b_o, a_d, b_d, mag_o, mag_d):
        layers, rank, _, part_o = a_o.shape
        sizes = (part_o, a_d.shape[3])
        columns = base_o.shape[2]
        depth = layers * rank
        base_o = pltpu.with_memory_space_constraint(base_o, pltpu.HBM)
        base_d = pltpu.with_memory_space_constraint(base_d, pltpu.HBM)
        shapes = (
            pltpu.VMEM(base_o.shape, BF16),
            pltpu.VMEM(base_d.shape, BF16),
            pltpu.VMEM((n, sum(sizes), depth), BF16),
            pltpu.VMEM((2, layers, depth, columns), BF16),
            pltpu.VMEM((2 * layers, columns), F32),
        )
        held_o, held_d, full_a, weights, scale = pl.pallas_call(
            functools.partial(gather_kernel, n, n_tp, sizes, rank),
            out_shape=shapes,
            in_specs=[anywhere] * 2 + [in_vmem] * 6,
            out_specs=[in_vmem] * 5,
            scratch_shapes=[
                pltpu.VMEM((sum(sizes), depth), BF16),
                pltpu.VMEM((2, layers, 8, columns), F32),
                pltpu.VMEM((2 * layers, columns), F32),
                pltpu.VMEM((n_tp - 1, 2 * layers, columns), F32),
                pltpu.SemaphoreType.DMA((2, layers, n)),
                pltpu.SemaphoreType.DMA,
                pltpu.SemaphoreType.DMA((3, n)),
                pltpu.SemaphoreType.DMA((n,)),
                pltpu.SemaphoreType.DMA((n_tp - 1,)),
                pltpu.SemaphoreType.DMA((n_tp - 1,)),
            ],
            compiler_params=pltpu.CompilerParams(
                collective_id=0, has_side_effects=True, vmem_limit_bytes=20 << 20
            ),
            name="gather_squares",
        )(
            base_o, base_d, a_o, a_d, b_o.swapaxes(1, 2), b_d.swapaxes(1, 2), mag_o, mag_d
        )

        kept = [
            pltpu.with_memory_space_constraint(x, pltpu.VMEM)
            for x in (held_o, held_d, full_a, weights, scale)
        ]
        return pl.pallas_call(
            functools.partial(finish_kernel, sizes),
            out_shape=[jax.ShapeDtypeStruct(b.shape, BF16) for b in (base_o, base_d)],
            grid=(layers, n),
            in_specs=[in_vmem] * 5,
            out_specs=[
                pl.BlockSpec((1, size, columns), lambda i, f: (i, f, 0)) for size in sizes
            ],
            compiler_params=pltpu.CompilerParams(vmem_limit_bytes=20 << 20),
            name="finish",
        )(*kept)

    return jax.shard_map(
        local,
        mesh=mesh,
        in_specs=(
            P(None, "tp", "fsdp"),
            P(None, "tp", "fsdp"),
            P(None, None, None, "fsdp"),
            P(None, "fsdp", None),
            P(None, None, None, "fsdp"),
            P(None, "fsdp", None),
            P(None, "fsdp"),
            P(None, "fsdp"),
        ),
        out_specs=(P(None, "tp", "fsdp"), P(None, "tp", "fsdp")),
        check_vma=False,
    )
```
